256 devices in a mesh: patch: 128 (over x, y, z), col: 2 (over core).
Axes of the slice: x: 4, y: 4, z: 8, core: 2. Of those that a mesh axis runs over, the one named last changes fastest.
Arguments:
- density: float32 [4, 131072], P(None, 'patch'), may hold values from -6 to 6
- block_values: bfloat16 [512, 32, 256, 256], P('patch', 'col'), may hold values from -0.09375 to 0.09375
- block_rows: int32 [512, 32], P('patch', 'col'), may hold values from 0 to 511, as said below
- block_counts: int32 [512], P('patch'), may hold values from 1 to 32
Outputs:
- potential: float32 [4, 131072], P(None, 'patch')
The draws below stay inside these ranges and needn't reach their ends.
Inputs may be any that keep to these rules, and one draw needn't show every extreme that they name: `block_rows`: slots of a block column at or past its count are padding and are not part of the matrix. Block row r belongs to owner r // 4. The slots held by one device (block columns of one patch owner, one col index, live or padding) name block rows of distinct owners in groups of exactly 2 slots a group, so at most 2 of them fall on one owner.
All inputs are finite; a program needn't handle non-finite values.
Results may differ from the reference program's by a relative error of at most 0.0027.
Values sent between devices are 32-bit elements; how exact they have to be, the bound alone decides.
No kernel may reach another device: no remote copies, remote signals or barrier semaphores. Data moves between devices by JAX's collectives and lax.ppermute only.
A program may use at most 64 MiB of HBM per device.

```python
import jax
import jax.numpy as jnp
from jax import lax

BS = 256
RHS = 4
LEVELS = 3
MAXB = 32
BLK_DEV = 4
NB = 512
NPANEL = 131072
CAP = 2
N_PATCH = 128
N_COL = 2


def draw_block_rows(key, part):
    slots = BLK_DEV * MAXB // N_COL
    devices = N_PATCH * N_COL
    keys = jax.random.split(jax.random.fold_in(key, 17), 3)
    owner_keys = jax.random.split(keys[0], devices)
    orders = jax.vmap(lambda sub: jax.random.permutation(sub, N_PATCH))(owner_keys)
    spot_keys = jax.random.split(keys[1], devices)
    spots = jax.vmap(lambda sub: jax.random.permutation(sub, slots))(spot_keys)
    groups = (spots // CAP).astype(jnp.int32)
    owners = jnp.take_along_axis(orders.astype(jnp.int32), groups, axis=1)
    within = jax.random.randint(keys[2], (devices, slots), 0, BLK_DEV, dtype=jnp.int32)
    rows = owners * BLK_DEV + within
    rows = rows.reshape(N_PATCH, N_COL, BLK_DEV, MAXB // N_COL).transpose(0, 2, 1, 3).reshape(NB, MAXB)
    return rows.astype(jnp.int32)


def with_ends(values, own_key, smallest, top_value):
    longest = values.shape.index(max(values.shape))
    spots = []
    for shift in (0, 1):
        where = [jax.random.randint(jax.random.fold_in(own_key, axis), (), 0, length) for axis, length in enumerate(values.shape)]
        where[longest] = (where[longest] + shift) % values.shape[longest]
        spots.append(tuple(where))
    return values.at[spots[0]].set(smallest).at[spots[1]].set(top_value)


def shard_levels(stream_key, shape, cuts, least, top_value):
    def one(position, blocks):
        draws = jax.random.uniform(jax.random.fold_in(jax.random.fold_in(stream_key, 6), position), (blocks,), jnp.float32, least / len(cuts), top_value / len(cuts))
        return jnp.repeat(jnp.exp(draws), shape[position] // blocks).reshape((-1,) + (1,) * (len(shape) - position - 1))

    level = one(*cuts[0])
    for cut in cuts[1:]:
        level = level * one(*cut)
    return level


def scatter_about(key, extent, deviation, most, cuts=(), kind=jnp.bfloat16):
    result = deviation * jax.random.normal(key, extent, jnp.float32)
    if cuts:
        result = result * shard_levels(key, extent, cuts, -0.22, 0.18)
    return jnp.clip(result, -most, most).astype(kind)


def setup_inputs(seed: int = 0) -> dict:
    splits = jax.random.split(jax.random.key(seed), 5)
    density = scatter_about(splits[0], (RHS, NPANEL), 1.0, 6.0, ((1, 128),), jnp.float32)
    block_values = scatter_about(splits[1], (NB, MAXB, BS, BS), (BS * MAXB // 2) ** -0.5, 0.09375, ((0, 128), (1, 2)))
    block_rows = draw_block_rows(jax.random.fold_in(splits[4], 71), 0)
    block_counts = with_ends(jax.random.randint(splits[3], (NB,), 1, MAXB + 1), jax.random.fold_in(splits[3], 1), 1, MAXB).astype(jnp.int32)
    return dict(density=density, block_values=block_values, block_rows=block_rows, block_counts=block_counts)


def forward_lift(density):
    smooth = density
    details = []
    for level_index in range(LEVELS):
        even_part = smooth[:, 0::2]
        odd_part = smooth[:, 1::2]
        zero_col = jnp.zeros_like(even_part[:, :1])
        even_next = jnp.concatenate([even_part[:, 1:], zero_col], axis=1)
        detail = odd_part - 0.5 * (even_part + even_next)
        detail_prior = jnp.concatenate([zero_col, detail[:, :-1]], axis=1)
        smooth = even_part + 0.25 * (detail_prior + detail)
        details.append(detail)
    return smooth, details


def owner_layout(pieces):
    parts = [piece.reshape(RHS, N_PATCH, -1) for piece in pieces]
    return jnp.concatenate(parts, axis=2).reshape(RHS, -1)


def inverse_lift(coefficients):
    local_len = BLK_DEV * BS
    local = coefficients.reshape(RHS, N_PATCH, local_len)
    coarse = local_len // (2 ** LEVELS)
    smooth = local[:, :, :coarse].reshape(RHS, -1)
    for level_index in range(LEVELS, 0, -1):
        lower = local_len // (2 ** level_index)
        upper = local_len // (2 ** (level_index - 1))
        detail = local[:, :, lower:upper].reshape(RHS, -1)
        zero_col = jnp.zeros_like(detail[:, :1])
        detail_prior = jnp.concatenate([zero_col, detail[:, :-1]], axis=1)
        even_part = smooth - 0.25 * (detail_prior + detail)
        even_next = jnp.concatenate([even_part[:, 1:], zero_col], axis=1)
        odd_part = detail + 0.5 * (even_part + even_next)
        smooth = jnp.stack([even_part, odd_part], axis=-1).reshape(RHS, -1)
    return smooth


def reference(density, block_values, block_rows, block_counts):
    smooth, details = forward_lift(density)
    coefficients = owner_layout([smooth] + details[::-1]).astype(jnp.bfloat16)
    blocks = coefficients.reshape(RHS, NB, BS).transpose(1, 0, 2)

    def apply_column(total, inputs):
        values, rows, count, vector = inputs
        terms = jnp.einsum("jkm,rm->jrk", values.astype(jnp.float32), vector.astype(jnp.float32), precision=lax.Precision.HIGHEST)
        live = (jnp.arange(MAXB, dtype=jnp.int32) < count).astype(jnp.float32)
        terms = terms * live[:, None, None]
        return total.at[rows].add(terms), None

    start = jnp.zeros((NB, RHS, BS), jnp.float32)
    applied, _ = lax.scan(apply_column, start, (block_values, block_rows, block_counts, blocks))
    flat = applied.transpose(1, 0, 2).reshape(RHS, -1)
    return 0.5 * density + inverse_lift(flat)
```

```python
import functools

import jax
import jax.numpy as jnp
from jax import lax
from jax.experimental import pallas as pl
from jax.experimental.pallas import tpu as pltpu
from jax.sharding import Mesh, PartitionSpec as P

LEVELS = 3
NX, NY, NZ, NC = 4, 4, 8, 2
PATCH = ("x", "y", "z")
ALL = ("x", "y", "z", "c")
OWNERS = NX * NY * NZ
REC = NZ + 1


def device_id(x, y, z, c):
    return ((x * NY + y) * NZ + z) * NC + c


def halo_pairs():
    pairs = []
    for p in range(OWNERS):
        pairs.append((p * NC, ((p + 1) % OWNERS) * NC))
        pairs.append((p * NC + 1, ((p - 1) % OWNERS) * NC + 1))
    return pairs


def line_pairs(shift, swap):
    pairs = []
    for x in range(NX):
        for y in range(NY):
            for z in range(NZ):
                for c in range(NC):
                    if (c == 0) != swap:
                        target = device_id((x + shift) % NX, y, z, c)
                    else:
                        target = device_id(x, (y + shift) % NY, z, c)
                    pairs.append((device_id(x, y, z, c), target))
    return pairs


def inside_mask(length, margin):
    where = (
        lax.axis_index(PATCH) * length + jnp.arange(length + 2 * margin, dtype=jnp.int32) - margin
    )
    valid = (where >= 0) & (where < OWNERS * length)
    return valid.astype(jnp.float32)[None, :]


def forward(density, left, right):
    local_len = density.shape[1]
    reach = 2 ** (LEVELS + 1)
    details = []
    smooth = jnp.concatenate([left[:, -reach:], density, right[:, :reach]], axis=1)
    for level_index in range(LEVELS):
        margin = reach // 2 ** (level_index + 1)
        length = local_len // 2 ** (level_index + 1)
        keep = inside_mask(length, margin)
        even_part = smooth[:, 0::2]
        odd_part = smooth[:, 1::2]
        zero_col = jnp.zeros_like(even_part[:, :1])
        even_next = jnp.concatenate([even_part[:, 1:], zero_col], axis=1)
        detail = (odd_part - 0.5 * (even_part + even_next)) * keep
        detail_prior = jnp.concatenate([zero_col, detail[:, :-1]], axis=1)
        smooth = (even_part + 0.25 * (detail_prior + detail)) * keep
        details.append(detail[:, margin : margin + length])
    smooth = smooth[:, margin : margin + length]
    return jnp.concatenate([smooth] + details[::-1], axis=1).astype(jnp.bfloat16)


def inverse(pieces, lefts, rights):
    sides = pieces[0].shape[0]
    zero = jnp.zeros((sides, 1), jnp.float32)
    extended = [
        jnp.concatenate([zero, left, piece, right, zero], axis=1)
        for left, piece, right in zip(lefts, pieces, rights)
    ]
    smooth = extended[0]
    for step_index in range(LEVELS):
        detail = extended[step_index + 1]
        length = detail.shape[1] - 4
        keep = inside_mask(length, 2)
        zero_col = jnp.zeros_like(detail[:, :1])
        detail_prior = jnp.concatenate([zero_col, detail[:, :-1]], axis=1)
        even_part = (smooth - 0.25 * (detail_prior + detail)) * keep
        even_next = jnp.concatenate([even_part[:, 1:], zero_col], axis=1)
        odd_part = detail + 0.5 * (even_part + even_next)
        smooth = jnp.stack([even_part, odd_part], axis=-1).reshape(sides, -1)[:, 2:-2]
    return smooth[:, 2:-2]


def terms_kernel(counts, core, vector, values, own, other):
    step = pl.program_id(0)
    chunk = values.shape[0]
    slots = (pl.num_programs(0) * chunk) // vector.shape[0]
    column = (step * chunk) // slots
    first = (step * chunk) % slots + core[0] * slots
    vec = vector[column]
    for index in range(chunk):
        term = lax.dot_general(
            vec, values[index], (((1,), (1,)), ((), ())), preferred_element_type=jnp.float32
        )
        term = jnp.where(first + index < counts[column], term[:4], 0.0)
        low, high = term[:, :128], term[:, 128:]
        own[index] = jnp.where(core[0] == 0, low, high)
        other[index] = jnp.where(core[0] == 0, high, low)


def terms(vector, values, counts, core):
    held = values.shape[0]
    chunk = 8
    smem = pl.BlockSpec(memory_space=pltpu.SMEM)
    block = jax.ShapeDtypeStruct((held, 4, 128), jnp.float32)
    return pl.pallas_call(
        terms_kernel,
        grid=(held // chunk,),
        in_specs=[
            smem,
            smem,
            pl.BlockSpec(vector.shape, lambda i: (0, 0, 0)),
            pl.BlockSpec((chunk, 256, 256), lambda i: (i, 0, 0)),
        ],
        out_specs=[pl.BlockSpec((chunk, 4, 128), lambda i: (i, 0, 0))] * 2,
        out_shape=[block, block],
        name="terms",
    )(counts, core, vector, values)


def relative(column_x, column_y, place):
    first = jnp.where(place[2] == 0, column_x - place[0], column_y - place[1])
    second = jnp.where(place[2] == 0, column_y - place[1], column_x - place[0])
    return (first & 3) * 4 + (second & 3)


def scatter_kernel(place, rows_own, rows_other, own, other, out0, out1, out2, out3, dense):
    dense[...] = jnp.zeros_like(dense)
    for rows, source in ((rows_own, own), (rows_other, other)):

        def add(index, carry):
            row = rows[index]
            owner = row >> 2
            column = relative(owner >> 5, (owner >> 3) & 3, place)
            spot = (column * REC + (owner & 7)) * 4 + (row & 3)
            dense[spot] = dense[spot] + source[index]
            return carry

        lax.fori_loop(0, source.shape[0], add, 0, unroll=8)
    lane = lax.broadcasted_iota(jnp.int32, (4, 128), 1)
    for first in range(4):
        for second in range(4):
            here = first * 4 + second
            x = (jnp.where(place[2] == 0, first, second) + place[0]) & 3
            y = (jnp.where(place[2] == 0, second, first) + place[1]) & 3
            column = x * 4 + y
            after = (column + 1) & 15
            before = (column + 15) & 15
            right = relative(after >> 2, after & 3, place) * REC * 4
            left = (relative(before >> 2, before & 3, place) * REC + 7) * 4
            for b in range(4):
                high = jnp.where(column == 15, 0.0, dense[right + b])
                low = jnp.where(column == 0, 0.0, dense[left + b])
                dense[(here * REC + NZ) * 4 + b] = jnp.where(lane < 64, high, low)
    size = out0.shape[0]
    for index, out in enumerate((out0, out1, out2, out3)):
        out[...] = dense[pl.ds(index * size, size)]


def scatter(place, rows_own, rows_other, own, other):
    size = 4 * REC * 4
    smem = pl.BlockSpec(memory_space=pltpu.SMEM)
    vmem = pl.BlockSpec(memory_space=pltpu.VMEM)
    return pl.pallas_call(
        scatter_kernel,
        in_specs=[smem] * 3 + [vmem] * 2,
        out_specs=[vmem] * 4,
        out_shape=[jax.ShapeDtypeStruct((size, 4, 128), jnp.float32)] * 4,
        scratch_shapes=[pltpu.VMEM((4 * size, 4, 128), jnp.float32)],
        name="scatter",
    )(place, rows_own, rows_other, own, other)


def body(density, block_values, block_rows, block_counts):
    sides, local_len = density.shape
    col_blocks, slots, block, _ = block_values.shape
    held = col_blocks * slots
    x, y, z, c = (lax.axis_index(axis) for axis in ALL)
    patch = lax.axis_index(PATCH)
    across = [(0, 1), (1, 0)]
    edge = jnp.where(c == 0, density[:, -128:], density[:, :128])
    halo = lax.ppermute(edge, ALL, halo_pairs())
    ids = jnp.concatenate(
        [block_rows.reshape(1, held).astype(jnp.float32), jnp.zeros((1, 128 - held), jnp.float32)], axis=1
    )
    swapped = lax.ppermute(jnp.concatenate([halo, ids], axis=0), "c", across)
    rows_other = swapped[4, :held].astype(jnp.int32)
    rows_own = block_rows.reshape(held)
    left = jnp.where(c == 0, halo, swapped[:4]) * (patch > 0).astype(jnp.float32)
    right = jnp.where(c == 0, swapped[:4], halo) * (patch < OWNERS - 1).astype(jnp.float32)

    vector = forward(density, left, right)
    blocks = vector.reshape(sides, col_blocks, block).transpose(1, 0, 2)
    blocks = jnp.concatenate([blocks, jnp.zeros_like(blocks)], axis=1)
    core = c.reshape(1).astype(jnp.int32)
    own, other = terms(blocks, block_values.reshape(held, block, block), block_counts, core)
    received = lax.ppermute(other, "c", across)
    place = jnp.stack([x, y, c]).astype(jnp.int32)
    parts = scatter(place, rows_own, rows_other, own, received)

    first = parts[0]
    for shift in (2, 1, 3):
        first = first + lax.ppermute(parts[shift], ALL, line_pairs(shift, False))
    first = first.reshape(4, REC, 16, 128)
    second = first[0]
    for shift in (2, 1, 3):
        second = second + lax.ppermute(first[shift], ALL, line_pairs(shift, True))
    lane = jnp.arange(128, dtype=jnp.int32)[None, None, :]
    ends = second[NZ:]
    mine = second[:NZ]
    after = jnp.concatenate([mine[1:], ends], axis=0)
    before = jnp.concatenate([ends, mine[:-1]], axis=0)
    message = jnp.concatenate([mine, jnp.where(lane < 64, after, before)], axis=1)
    last = lax.all_to_all(message, "z", 0, 0, tiled=True).sum(axis=0)
    peer = lax.ppermute(last, "c", across)
    zero_half = jnp.where(c == 0, last, peer).reshape(2, 4, 4, 128)
    one_half = jnp.where(c == 0, peer, last).reshape(2, 4, 4, 128)
    a, ga = zero_half[0], zero_half[1]
    d, gd = one_half[0], one_half[1]
    pieces = [
        a[0],
        d[0],
        jnp.concatenate([a[1], d[1]], axis=1),
        jnp.concatenate([a[2], d[2], a[3], d[3]], axis=1),
    ]
    zero = jnp.zeros((sides, 1), jnp.float32)
    lefts = [zero, gd[0][:, 127:], gd[1][:, 127:], gd[3][:, 127:]]
    rights = [ga[0][:, :1], gd[0][:, :1], ga[1][:, :1], ga[2][:, :1]]
    return 0.5 * density + inverse(pieces, lefts, rights)


def solution(mesh):
    grid = Mesh(mesh.devices.reshape(NX, NY, NZ, NC), ALL)
    return jax.shard_map(
        body,
        mesh=grid,
        in_specs=(P(None, PATCH), P(PATCH, "c", None, None), P(PATCH, "c"), P(PATCH)),
        out_specs=P(None, PATCH),
        check_vma=False,
    )
```

```python
import jax
import jax.numpy as jnp
import numpy as np
from jax import lax
from jax.experimental import pallas as pl
from jax.experimental.pallas import tpu as pltpu
from jax.sharding import Mesh, PartitionSpec as P

LEVELS = 3
NX, NY, NZ, NC = 4, 4, 8, 2
PATCH = ("x", "y", "z")
ALL = ("x", "y", "z", "c")
OWNERS = NX * NY * NZ
TILES = 2 * NZ + 2
COLS, SLOTS, BS = 4, 16, 256
HELD = COLS * SLOTS
LEN = COLS * BS
REACH = 16
SMALL = 4 * 1024 * 1024


def device_id(x, y, z, c):
    return ((x * NY + y) * NZ + z) * NC + c


def halo_pairs():
    pairs = []
    for p in range(OWNERS):
        pairs.append((p * NC, ((p + 1) % OWNERS) * NC))
        pairs.append((p * NC + 1, ((p - 1) % OWNERS) * NC + 1))
    return pairs


def line_pairs(shift, swap):
    pairs = []
    for x in range(NX):
        for y in range(NY):
            for z in range(NZ):
                for c in range(NC):
                    if (c == 0) != swap:
                        target = device_id((x + shift) % NX, y, z, c)
                    else:
                        target = device_id(x, (y + shift) % NY, z, c)
                    pairs.append((device_id(x, y, z, c), target))
    return pairs


def edge_table():
    table = np.zeros((128, 128), np.float32)
    for at_end in (False, True):
        for unit in range(64):
            line = np.zeros(LEN + 2 * REACH)
            where = unit if unit < 32 else LEN + unit - 32
            line[where] = 1.0
            if at_end:
                line[:REACH] = 0.0
                line[REACH + LEN :] = 0.0
            smooth, details = line, []
            for level in range(LEVELS):
                margin, length = REACH >> (level + 1), LEN >> (level + 1)
                keep = np.ones(length + 2 * margin)
                if at_end:
                    keep[:margin] = 0.0
                    keep[margin + length :] = 0.0
                even, odd = smooth[0::2], smooth[1::2]
                detail = (odd - 0.5 * (even + np.append(even[1:], 0.0))) * keep
                smooth = (even + 0.25 * (np.append(0.0, detail[:-1]) + detail)) * keep
                details.append(detail[margin : margin + length])
            s3 = smooth[margin : margin + length]
            d1, d2, d3 = details
            values = [s3[0], d3[0], d3[127], d2[0], d2[255], d1[511]]
            table[unit, 8 * at_end : 8 * at_end + 6] = values
    return table


def coordinates():
    return [lax.axis_index(axis) for axis in ALL]


def terms_kernel(counts, density, values, own, send, wide, xt, d1, s1, d2, s2, d3, vec, acc, held, sems):
    core = lax.axis_index("c")
    parts = 8
    size = HELD // parts
    copies = [
        pltpu.make_async_copy(values.at[pl.ds(i * size, size)], held.at[pl.ds(i * size, size)], sems.at[i])
        for i in range(parts)
    ]
    for copy in copies:
        copy.start()
    wide[0:4, :] = density[...]
    wide[4:8, :] = density[...]
    for group in range(8):
        tile = wide[:, pl.ds(group * 128, 128)]
        xt[pl.ds(8 + group * 128, 128), :] = jnp.concatenate([tile] * 16, axis=0).T
    pad = jnp.zeros((8, 128), jnp.float32)

    def lift(source, length, detail, smooth, fix):
        source[pl.ds(8 + 2 * length, 8), :] = pad
        detail[0:8, :] = pad
        step = min(length, 128)
        for start in range(0, length, step):
            even = source[pl.ds(8 + 2 * start, step, stride=2), :]
            odd = source[pl.ds(9 + 2 * start, step, stride=2), :]
            after = source[pl.ds(10 + 2 * start, step, stride=2), :]
            detail[pl.ds(8 + start, step), :] = odd - 0.5 * (even + after)
        if fix:
            row = lax.broadcasted_iota(jnp.int32, (8, 128), 0)
            detail[8:16, :] = jnp.where(row == 0, 0.0, detail[8:16, :])
            detail[pl.ds(length, 8), :] = jnp.where(row == 7, 0.0, detail[pl.ds(length, 8), :])
        for start in range(0, length, step):
            even = source[pl.ds(8 + 2 * start, step, stride=2), :]
            low = detail[pl.ds(7 + start, step), :]
            high = detail[pl.ds(8 + start, step), :]
            smooth(start, step, even + 0.25 * (low + high))

    lane = lax.broadcasted_iota(jnp.int32, (8, 128), 1) & 7
    row = lax.broadcasted_iota(jnp.int32, (8, 128), 0)

    def put(at, value):
        count = value.shape[0]
        lanes = lax.broadcasted_iota(jnp.int32, (count, 128), 1) & 7
        vec[pl.ds(at, count), :] = jnp.where(lanes < 4, value, 0.0)

    def keep1(start, step, value):
        s1[pl.ds(8 + start, step), :] = value

    def keep2(start, step, value):
        s2[pl.ds(8 + start, step), :] = value

    lift(xt, 512, d1, keep1, False)
    lift(s1, 256, d2, keep2, False)
    lift(s2, 128, d3, lambda start, step, value: put(start, value), True)
    put(128, d3[8:136, :])
    put(256, d2[8:264, :])
    for start in range(0, 512, 128):
        put(512 + start, d1[pl.ds(8 + start, 128), :])

    def patch(at, which, lanes_weights, clear):
        tile = vec[pl.ds(at, 8), :]
        if clear:
            tile = jnp.where((row == which) & (lane < 4), 0.0, tile)
        for index, at_row, weight in lanes_weights:
            tile = jnp.where((row == at_row) & (lane == index), weight, tile)
        vec[pl.ds(at, 8), :] = tile

    patch(0, 0, [(4, 0, 1.0), (5, 1, 0.25)], True)
    patch(120, 7, [(6, 7, 0.25)], False)
    patch(128, 0, [(5, 0, 1.0)], True)
    patch(248, 7, [(6, 7, 1.0)], True)
    patch(256, 0, [(4, 0, 1.0)], True)
    patch(504, 7, [(5, 7, 1.0)], True)
    patch(1016, 7, [(4, 7, 1.0)], True)

    whose = lax.broadcasted_iota(jnp.int32, (1, 128), 1) >> 3
    for column in range(COLS):
        vector = vec[pl.ds(column * BS, BS), :].astype(jnp.bfloat16)
        total = None
        for slot in range(SLOTS):
            index = column * SLOTS + slot
            if index % size == 0:
                copies[index // size].wait()
            live = core * SLOTS + slot < counts[column]
            mask = (whose == jnp.where(live, slot, -1)).astype(jnp.float32).astype(jnp.bfloat16)
            part = jnp.dot(held[index], vector * mask, preferred_element_type=jnp.float32)
            if slot == 0:
                acc[...] = part
            else:
                acc[...] += part
        turned = acc[...].T
        low = turned[:, :128].reshape(SLOTS, 8, 128)
        high = turned[:, 128:].reshape(SLOTS, 8, 128)
        at = pl.ds(column * SLOTS, SLOTS)
        own[at] = jnp.where(core == 0, low, high)
        send[at] = jnp.where(core == 0, high, low)


def terms(counts, density, values):
    smem = pl.BlockSpec(memory_space=pltpu.SMEM)
    vmem = pl.BlockSpec(memory_space=pltpu.VMEM)
    block = jax.ShapeDtypeStruct((HELD, 8, 128), jnp.float32)
    f32 = jnp.float32
    return pl.pallas_call(
        terms_kernel,
        in_specs=[smem, vmem, pl.BlockSpec(memory_space=pltpu.HBM)],
        out_specs=[vmem, vmem],
        out_shape=[block, block],
        scratch_shapes=[
            pltpu.VMEM((8, LEN), f32),
            pltpu.VMEM((LEN + 16, 128), f32),
            pltpu.VMEM((512 + 16, 128), f32),
            pltpu.VMEM((512 + 16, 128), f32),
            pltpu.VMEM((256 + 16, 128), f32),
            pltpu.VMEM((256 + 16, 128), f32),
            pltpu.VMEM((128 + 16, 128), f32),
            pltpu.VMEM((LEN, 128), f32),
            pltpu.VMEM((BS, 128), f32),
            pltpu.VMEM((HELD, BS, BS), jnp.bfloat16),
            pltpu.SemaphoreType.DMA((8,)),
        ],
        compiler_params=pltpu.CompilerParams(vmem_limit_bytes=16 * 1024 * 1024),
        cost_estimate=pl.CostEstimate(
            flops=2 * HELD * BS * BS * 128, bytes_accessed=2 * HELD * BS * BS, transcendentals=0
        ),
        name="terms",
    )(counts, density, values)


def edges_kernel(density, mine, other, table, out):
    x, y, z, core = coordinates()
    left = jnp.where(core == 0, mine[...], other[...])
    right = jnp.where(core == 0, other[...], mine[...])
    lane = lax.broadcasted_iota(jnp.int32, (4, 128), 1)
    first = density[:, 0:128]
    last = density[:, LEN - 128 :]
    inputs = jnp.where(
        lane < 32,
        jnp.where(lane < 16, pltpu.roll(left, 16, 1), pltpu.roll(first, 16, 1)),
        jnp.where(lane < 48, pltpu.roll(last, 48, 1), pltpu.roll(right, 48, 1)),
    )
    inputs = jnp.where(lane < 64, inputs, 0.0)
    values = jnp.dot(
        inputs, table[...], precision=lax.Precision.HIGHEST, preferred_element_type=jnp.float32
    )
    patch = (x * NY + y) * NZ + z
    low = (lane == 0) | (lane == 1) | (lane == 3)
    at_end = jnp.where(low, (patch == 0).astype(jnp.int32), (patch == OWNERS - 1).astype(jnp.int32))
    values = jnp.where(at_end == 1, pltpu.roll(values, 120, 1), values)
    values = values.astype(jnp.bfloat16).astype(jnp.float32)
    for index in range(6):
        spread = jnp.broadcast_to(values[:, index : index + 1], (4, 128))
        out[index, 0:4, :] = spread
        out[index, 4:8, :] = jnp.zeros((4, 128), jnp.float32)


def edges(density, mine, other, table):
    vmem = pl.BlockSpec(memory_space=pltpu.VMEM)
    return pl.pallas_call(
        edges_kernel,
        in_specs=[vmem] * 4,
        out_specs=vmem,
        out_shape=jax.ShapeDtypeStruct((6, 8, 128), jnp.float32),
        compiler_params=pltpu.CompilerParams(vmem_limit_bytes=SMALL),
        cost_estimate=pl.CostEstimate(flops=10**6, bytes_accessed=10**5, transcendentals=0),
        name="edges",
    )(density, mine, other, table)


def scatter_kernel(rows_own, rows_other, own, other, edge, out0, out1, out2, out3, dense, staged, base):
    x, y, _, core = coordinates()

    def relative(column_x, column_y):
        dx, dy = (column_x - x) & 3, (column_y - y) & 3
        return jnp.where(core == 0, dx * 4 + dy, dy * 4 + dx)

    for column in range(16):
        base[column] = relative(column >> 2, column & 3) * TILES
    dense[...] = jnp.zeros_like(dense)
    sub = lax.broadcasted_iota(jnp.int32, (SLOTS, 8, 128), 1)
    which = ((0, 1, 2), (3, 4), (), (5,))
    for side, source in enumerate((own, other)):
        for column in range(COLS):
            tile = source[pl.ds(column * SLOTS, SLOTS)]
            total = tile
            for place, index in enumerate(which[column]):
                total = total + tile[:, 4 + place : 5 + place, :] * edge[index][None]
            total = jnp.where(sub < 4, total, 0.0)
            at = pl.ds((side * COLS + column) * SLOTS, SLOTS)
            staged[0, at] = total
            staged[1, at] = pltpu.roll(total, 4, 1)
    for side, rows in enumerate((rows_own, rows_other)):
        for column in range(COLS):
            for slot in range(SLOTS):
                number = rows[column, slot]
                spot = base[number >> 5] + ((number >> 1) & 15)
                value = staged[number & 1, (side * COLS + column) * SLOTS + slot]
                dense[spot] = dense[spot] + value
    lane = lax.broadcasted_iota(jnp.int32, (2, 8, 128), 2)
    for first in range(4):
        for second in range(4):
            here = (first * 4 + second) * TILES
            cx = (jnp.where(core == 0, first, second) + x) & 3
            cy = (jnp.where(core == 0, second, first) + y) & 3
            column = cx * 4 + cy
            high = jnp.where(column == 15, 0.0, dense[pl.ds(base[(column + 1) & 15], 2)])
            low = jnp.where(column == 0, 0.0, dense[pl.ds(base[(column + 15) & 15] + 14, 2)])
            dense[pl.ds(here + 2 * NZ, 2)] = jnp.where(lane < 64, high, low)
    size = 4 * TILES
    for index, out in enumerate((out0, out1, out2, out3)):
        out[...] = dense[pl.ds(index * size, size)]


def scatter(rows_own, rows_other, own, other, edge):
    size = 4 * TILES
    smem = pl.BlockSpec(memory_space=pltpu.SMEM)
    vmem = pl.BlockSpec(memory_space=pltpu.VMEM)
    return pl.pallas_call(
        scatter_kernel,
        in_specs=[smem] * 2 + [vmem] * 3,
        out_specs=[vmem] * 4,
        out_shape=[jax.ShapeDtypeStruct((size, 8, 128), jnp.float32)] * 4,
        scratch_shapes=[
            pltpu.VMEM((4 * size, 8, 128), jnp.float32),
            pltpu.VMEM((2, 2 * HELD, 8, 128), jnp.float32),
            pltpu.SMEM((16,), jnp.int32),
        ],
        compiler_params=pltpu.CompilerParams(vmem_limit_bytes=2 * SMALL),
        cost_estimate=pl.CostEstimate(flops=10**6, bytes_accessed=10**6, transcendentals=0),
        name="scatter",
    )(rows_own, rows_other, own, other, edge)


def messages_kernel(part0, part1, part2, part3, keep, send, total):
    z = lax.axis_index("z")
    total[...] = (part0[...] + part1[...]) + (part2[...] + part3[...])
    lane = lax.broadcasted_iota(jnp.int32, (2, 8, 128), 2)
    for out, parity in ((keep, z & 1), (send, 1 - (z & 1))):
        for index in range(4):
            owner = (((z >> 1) + index) & 3) * 2 + parity
            after = jnp.where(owner == NZ - 1, NZ, owner + 1)
            before = jnp.where(owner == 0, NZ, owner - 1)
            out[index, 0:2] = total[pl.ds(owner * 2, 2)]
            out[index, 2:4] = jnp.where(
                lane < 64, total[pl.ds(after * 2, 2)], total[pl.ds(before * 2, 2)]
            )


def messages(parts):
    vmem = pl.BlockSpec(memory_space=pltpu.VMEM)
    return pl.pallas_call(
        messages_kernel,
        in_specs=[vmem] * 4,
        out_specs=[vmem] * 2,
        out_shape=[jax.ShapeDtypeStruct((4, 4, 8, 128), jnp.float32)] * 2,
        scratch_shapes=[pltpu.VMEM((TILES, 8, 128), jnp.float32)],
        compiler_params=pltpu.CompilerParams(vmem_limit_bytes=SMALL),
        cost_estimate=pl.CostEstimate(flops=10**5, bytes_accessed=10**5, transcendentals=0),
        name="messages",
    )(*parts)


def inverse_kernel(density, mine, peer, out, turned, s3, s2, s1, s0, d3, d2, d1, even):
    x, y, z, core = coordinates()
    last = ((x * NY + y) * NZ + z) == OWNERS - 1
    inside = jnp.where(last, 0.0, 1.0)
    first = jnp.where(core == 0, mine[...], peer[...])
    second = jnp.where(core == 0, peer[...], mine[...])
    both = jnp.concatenate([first, second, jnp.zeros((64, 128), jnp.float32)], axis=0)
    turned[...] = both.T

    def piece(half, block):
        return pltpu.roll(turned[...], (128 - (half * 32 + block * 4)) % 128, 1)

    def ghost(half, block, top):
        tile = turned[0:8, :] if top else turned[120:128, :]
        return pltpu.roll(tile, (128 - (half * 32 + 16 + block * 4)) % 128, 1)

    def fill(target, length, parts, left, right):
        for index, (half, block) in enumerate(parts):
            target[pl.ds(8 + index * 128, 128), :] = piece(half, block)
        if left is not None:
            target[0:8, :] = ghost(left[0], left[1], False)
        target[pl.ds(8 + length, 8), :] = ghost(right[0], right[1], True)

    fill(s3, 128, [(0, 0)], None, (0, 0))
    fill(d3, 128, [(1, 0)], (1, 0), (1, 0))
    fill(d2, 256, [(0, 1), (1, 1)], (1, 1), (0, 1))
    fill(d1, 512, [(0, 2), (1, 2), (0, 3), (1, 3)], (1, 3), (0, 2))

    def level(smooth, detail, length, target):
        for start in range(0, length, 128):
            value = smooth[pl.ds(8 + start, 128), :] - 0.25 * (
                detail[pl.ds(7 + start, 128), :] + detail[pl.ds(8 + start, 128), :]
            )
            even[pl.ds(start, 128), :] = value
            target[pl.ds(8 + 2 * start, 128, stride=2), :] = value
        tail = inside * (
            smooth[pl.ds(8 + length, 8), :]
            - 0.25 * (detail[pl.ds(7 + length, 8), :] + detail[pl.ds(8 + length, 8), :])
        )
        even[pl.ds(length, 8), :] = tail
        target[pl.ds(8 + 2 * length, 8), :] = tail
        for start in range(0, length, 128):
            value = detail[pl.ds(8 + start, 128), :] + 0.5 * (
                even[pl.ds(start, 128), :] + even[pl.ds(start + 1, 128), :]
            )
            target[pl.ds(9 + 2 * start, 128, stride=2), :] = value

    level(s3, d3, 128, s2)
    level(s2, d2, 256, s1)
    level(s1, d1, 512, s0)
    for group in range(8):
        at = pl.ds(group * 128, 128)
        out[:, at] = 0.5 * density[:, at] + s0[pl.ds(8 + group * 128, 128), :].T[0:4, :]


def inverse(density, mine, peer):
    vmem = pl.BlockSpec(memory_space=pltpu.VMEM)
    f32 = jnp.float32
    return pl.pallas_call(
        inverse_kernel,
        in_specs=[vmem] * 3,
        out_specs=vmem,
        out_shape=jax.ShapeDtypeStruct(density.shape, f32),
        scratch_shapes=[pltpu.VMEM((128, 128), f32)]
        + [pltpu.VMEM((n + 16, 128), f32) for n in (128, 256, 512, 1024, 128, 256, 512, 512)],
        compiler_params=pltpu.CompilerParams(vmem_limit_bytes=2 * SMALL),
        cost_estimate=pl.CostEstimate(flops=10**6, bytes_accessed=10**5, transcendentals=0),
        name="inverse",
    )(density, mine, peer)


def body(density, block_values, block_rows, block_counts):
    core = lax.axis_index("c")
    across = [(0, 1), (1, 0)]
    edge = jnp.where(core == 0, density[:, -128:], density[:, :128])
    halo = lax.ppermute(edge, ALL, halo_pairs())
    rows_other = lax.ppermute(block_rows, "c", across)
    own, send = terms(block_counts, density, block_values.reshape(HELD, BS, BS))
    received = lax.ppermute(send, "c", across)
    halo_other = lax.ppermute(halo, "c", across)
    edge_values = edges(density, halo, halo_other, jnp.asarray(edge_table()))
    parts = scatter(block_rows, rows_other, own, received, edge_values)

    first = parts[0]
    for shift in (2, 1, 3):
        first = first + lax.ppermute(parts[shift], ALL, line_pairs(shift, False))
    first = first.reshape(4, TILES, 8, 128)
    second = [first[0]]
    for shift in (2, 1, 3):
        second.append(lax.ppermute(first[shift], ALL, line_pairs(shift, True)))
    keep, away = messages(second)
    keep = keep + lax.ppermute(away, "z", [(i, i ^ 1) for i in range(NZ)])
    last = keep[0]
    for shift in (2, 1, 3):
        last = last + lax.ppermute(keep[shift], "z", [(i, (i + 2 * shift) % NZ) for i in range(NZ)])
    last = last.reshape(32, 128)
    return inverse(density, last, lax.ppermute(last, "c", across))


def solution(mesh):
    grid = Mesh(mesh.devices.reshape(NX, NY, NZ, NC), ALL)
    return jax.shard_map(
        body,
        mesh=grid,
        in_specs=(P(None, PATCH), P(PATCH, "c", None, None), P(PATCH, "c"), P(PATCH)),
        out_specs=P(None, PATCH),
        check_vma=False,
    )
```

```python
import jax
import jax.numpy as jnp
import numpy as np
from jax import lax
from jax.experimental import pallas as pl
from jax.experimental.pallas import tpu as pltpu
from jax.sharding import Mesh, PartitionSpec as P


LEVELS = 3
NX, NY, NZ, NC = 4, 4, 8, 2
PATCH = ("x", "y", "z")
ALL = ("x", "y", "z", "c")
OWNERS = NX * NY * NZ
TILES = 2 * NZ + 1
COLS, SLOTS, BS = 4, 16, 256
HELD = COLS * SLOTS
LEN = COLS * BS
REACH = 16
SMALL = 4 * 1024 * 1024


def device_id(x, y, z, c):
    return ((x * NY + y) * NZ + z) * NC + c


def halo_pairs():
    pairs = []
    for p in range(OWNERS):
        pairs.append((p * NC, ((p + 1) % OWNERS) * NC))
        pairs.append((p * NC + 1, ((p - 1) % OWNERS) * NC + 1))
    return pairs


def stage_kernel(density, staged, edge):
    core = lax.axis_index("c")
    value = density[...]
    staged[...] = value
    edge[...] = jnp.where(core == 0, value[:, LEN - 128 :], value[:, :128])


def stage(density):
    vmem = pl.BlockSpec(memory_space=pltpu.VMEM)
    return pl.pallas_call(
        stage_kernel,
        in_specs=[vmem],
        out_specs=[vmem, vmem],
        out_shape=[
            jax.ShapeDtypeStruct(density.shape, jnp.float32),
            jax.ShapeDtypeStruct((4, 128), jnp.float32),
        ],
        compiler_params=pltpu.CompilerParams(vmem_limit_bytes=SMALL),
        name="stage",
    )(density)


def pack_edges(after, before):
    lane = lax.broadcasted_iota(jnp.int32, (8, 128), 1)
    tiles = [jnp.where(lane < 64, high, low) for high, low in zip(after, before)]
    return jnp.where((lane >= 16) & (lane < 48), pltpu.roll(tiles[1], 32, 1), tiles[0])


def unpack_edges(tile):
    return tile, pltpu.roll(tile, 96, 1)


def line_pairs(shift, swap):
    pairs = []
    for x in range(NX):
        for y in range(NY):
            for z in range(NZ):
                for c in range(NC):
                    if (c == 0) != swap:
                        target = device_id((x + shift) % NX, y, z, c)
                    else:
                        target = device_id(x, (y + shift) % NY, z, c)
                    pairs.append((device_id(x, y, z, c), target))
    return pairs


def edge_table():
    table = np.zeros((128, 128), np.float32)
    for at_end in (False, True):
        for unit in range(64):
            line = np.zeros(LEN + 2 * REACH)
            where = unit if unit < 32 else LEN + unit - 32
            line[where] = 1.0
            if at_end:
                line[:REACH] = 0.0
                line[REACH + LEN :] = 0.0
            smooth, details = line, []
            for level in range(LEVELS):
                margin, length = REACH >> (level + 1), LEN >> (level + 1)
                keep = np.ones(length + 2 * margin)
                if at_end:
                    keep[:margin] = 0.0
                    keep[margin + length :] = 0.0
                even, odd = smooth[0::2], smooth[1::2]
                detail = (odd - 0.5 * (even + np.append(even[1:], 0.0))) * keep
                smooth = (even + 0.25 * (np.append(0.0, detail[:-1]) + detail)) * keep
                details.append(detail[margin : margin + length])
            s3 = smooth[margin : margin + length]
            d1, d2, d3 = details
            values = [s3[0], d3[0], d3[127], d2[0], d2[255], d1[511]]
            table[unit, 8 * at_end : 8 * at_end + 6] = values
    return table


def coordinates():
    return [lax.axis_index(axis) for axis in ALL]


CHUNKS = {0: 4, 4: 12, 16: 16, 32: 16, 48: 16}


def terms_kernel(density, values, own, send, wide, xt, d1, s1, d2, s2, d3, vec, acc, held, sems):
    core = lax.axis_index("c")
    copies = {
        at: pltpu.make_async_copy(values.at[pl.ds(at, size)], held.at[pl.ds(at, size)], sems.at[i])
        for i, (at, size) in enumerate(CHUNKS.items())
    }
    for copy in copies.values():
        copy.start()
    wide[0:4, :] = density[...]
    wide[4:8, :] = density[...]
    for group in range(8):
        tile = wide[:, pl.ds(group * 128, 128)]
        xt[pl.ds(8 + group * 128, 128), :] = jnp.concatenate([tile] * 16, axis=0).T
    pad = jnp.zeros((8, 128), jnp.float32)

    def lift(source, length, detail, smooth, fix):
        source[pl.ds(8 + 2 * length, 8), :] = pad
        detail[0:8, :] = pad
        step = min(length, 128)
        for start in range(0, length, step):
            even = source[pl.ds(8 + 2 * start, step, stride=2), :]
            odd = source[pl.ds(9 + 2 * start, step, stride=2), :]
            after = source[pl.ds(10 + 2 * start, step, stride=2), :]
            detail[pl.ds(8 + start, step), :] = odd - 0.5 * (even + after)
        if fix:
            row = lax.broadcasted_iota(jnp.int32, (8, 128), 0)
            detail[8:16, :] = jnp.where(row == 0, 0.0, detail[8:16, :])
            detail[pl.ds(length, 8), :] = jnp.where(row == 7, 0.0, detail[pl.ds(length, 8), :])
        for start in range(0, length, step):
            even = source[pl.ds(8 + 2 * start, step, stride=2), :]
            low = detail[pl.ds(7 + start, step), :]
            high = detail[pl.ds(8 + start, step), :]
            smooth(start, step, even + 0.25 * (low + high))

    lane = lax.broadcasted_iota(jnp.int32, (8, 128), 1) & 7
    row = lax.broadcasted_iota(jnp.int32, (8, 128), 0)

    def put(at, value):
        count = value.shape[0]
        lanes = lax.broadcasted_iota(jnp.int32, (count, 128), 1) & 7
        vec[pl.ds(at, count), :] = jnp.where(lanes < 4, value, 0.0)

    def keep1(start, step, value):
        s1[pl.ds(8 + start, step), :] = value

    def keep2(start, step, value):
        s2[pl.ds(8 + start, step), :] = value

    lift(xt, 512, d1, keep1, False)
    lift(s1, 256, d2, keep2, False)
    lift(s2, 128, d3, lambda start, step, value: put(start, value), True)
    put(128, d3[8:136, :])
    put(256, d2[8:264, :])
    for start in range(0, 512, 128):
        put(512 + start, d1[pl.ds(8 + start, 128), :])

    def patch(at, which, lanes_weights, clear):
        tile = vec[pl.ds(at, 8), :]
        if clear:
            tile = jnp.where((row == which) & (lane < 4), 0.0, tile)
        for index, at_row, weight in lanes_weights:
            tile = jnp.where((row == at_row) & (lane == index), weight, tile)
        vec[pl.ds(at, 8), :] = tile

    patch(0, 0, [(4, 0, 1.0), (5, 1, 0.25)], True)
    patch(120, 7, [(6, 7, 0.25)], False)
    patch(128, 0, [(5, 0, 1.0)], True)
    patch(248, 7, [(6, 7, 1.0)], True)
    patch(256, 0, [(4, 0, 1.0)], True)
    patch(504, 7, [(5, 7, 1.0)], True)
    patch(1016, 7, [(4, 7, 1.0)], True)

    whose = lax.broadcasted_iota(jnp.int32, (1, 128), 1) >> 3
    for column in range(COLS):
        vector = vec[pl.ds(column * BS, BS), :].astype(jnp.bfloat16)
        for slot in range(SLOTS):
            index = column * SLOTS + slot
            if index in copies:
                copies[index].wait()
            mask = (whose == slot).astype(jnp.float32).astype(jnp.bfloat16)
            part = jnp.dot(held[index], vector * mask, preferred_element_type=jnp.float32)
            if slot == 0:
                acc[...] = part
            else:
                acc[...] += part
        turned = acc[...].T
        low = turned[:, :128].reshape(SLOTS, 8, 128)
        high = turned[:, 128:].reshape(SLOTS, 8, 128)
        at = pl.ds(column * SLOTS, SLOTS)
        own[at] = jnp.where(core == 0, low, high)
        send[at] = jnp.where(core == 0, high, low)


def terms(density, values):
    vmem = pl.BlockSpec(memory_space=pltpu.VMEM)
    block = jax.ShapeDtypeStruct((HELD, 8, 128), jnp.float32)
    f32 = jnp.float32
    return pl.pallas_call(
        terms_kernel,
        in_specs=[vmem, pl.BlockSpec(memory_space=pltpu.HBM)],
        out_specs=[vmem, vmem],
        out_shape=[block, block],
        scratch_shapes=[
            pltpu.VMEM((8, LEN), f32),
            pltpu.VMEM((LEN + 16, 128), f32),
            pltpu.VMEM((512 + 16, 128), f32),
            pltpu.VMEM((512 + 16, 128), f32),
            pltpu.VMEM((256 + 16, 128), f32),
            pltpu.VMEM((256 + 16, 128), f32),
            pltpu.VMEM((128 + 16, 128), f32),
            pltpu.VMEM((LEN, 128), f32),
            pltpu.VMEM((BS, 128), f32),
            pltpu.VMEM((HELD, BS, BS), jnp.bfloat16),
            pltpu.SemaphoreType.DMA((len(CHUNKS),)),
        ],
        compiler_params=pltpu.CompilerParams(vmem_limit_bytes=50 * 1024 * 1024),
        cost_estimate=pl.CostEstimate(
            flops=2 * HELD * BS * BS * 128, bytes_accessed=2 * HELD * BS * BS, transcendentals=0
        ),
        name="terms",
    )(density, values)


def edges_kernel(density, mine, other, table, out):
    x, y, z, core = coordinates()
    left = jnp.where(core == 0, mine[...], other[...])
    right = jnp.where(core == 0, other[...], mine[...])
    lane = lax.broadcasted_iota(jnp.int32, (4, 128), 1)
    first = density[:, 0:128]
    last = density[:, LEN - 128 :]
    inputs = jnp.where(
        lane < 32,
        jnp.where(lane < 16, pltpu.roll(left, 16, 1), pltpu.roll(first, 16, 1)),
        jnp.where(lane < 48, pltpu.roll(last, 48, 1), pltpu.roll(right, 48, 1)),
    )
    inputs = jnp.where(lane < 64, inputs, 0.0)
    values = jnp.dot(
        inputs, table[...], precision=lax.Precision.HIGHEST, preferred_element_type=jnp.float32
    )
    patch = (x * NY + y) * NZ + z
    low = (lane == 0) | (lane == 1) | (lane == 3)
    at_end = jnp.where(low, (patch == 0).astype(jnp.int32), (patch == OWNERS - 1).astype(jnp.int32))
    values = jnp.where(at_end == 1, pltpu.roll(values, 120, 1), values)
    values = values.astype(jnp.bfloat16).astype(jnp.float32)
    for index in range(6):
        spread = jnp.broadcast_to(values[:, index : index + 1], (4, 128))
        out[index, 0:4, :] = spread
        out[index, 4:8, :] = jnp.zeros((4, 128), jnp.float32)


def edges(density, mine, other, table):
    vmem = pl.BlockSpec(memory_space=pltpu.VMEM)
    return pl.pallas_call(
        edges_kernel,
        in_specs=[vmem] * 4,
        out_specs=vmem,
        out_shape=jax.ShapeDtypeStruct((6, 8, 128), jnp.float32),
        compiler_params=pltpu.CompilerParams(vmem_limit_bytes=SMALL),
        cost_estimate=pl.CostEstimate(flops=10**6, bytes_accessed=10**5, transcendentals=0),
        name="edges",
    )(density, mine, other, table)


def scatter_kernel(
    counts_ref,
    rows_ref,
    rows_other_ref,
    own,
    other,
    edge,
    out0,
    out1,
    out2,
    out3,
    dense,
    staged,
    base,
    counts,
    rows_own,
    rows_other,
    sems,
):
    x, y, _, core = coordinates()
    copies = [
        pltpu.make_async_copy(rows_ref, rows_own, sems.at[0]),
        pltpu.make_async_copy(rows_other_ref, rows_other, sems.at[1]),
        pltpu.make_async_copy(counts_ref, counts, sems.at[2]),
    ]
    for copy in copies:
        copy.start()

    def relative(column_x, column_y):
        dx, dy = (column_x - x) & 3, (column_y - y) & 3
        return jnp.where(core == 0, dx * 4 + dy, dy * 4 + dx)

    for column in range(16):
        base[column] = relative(column >> 2, column & 3) * TILES
    dense[...] = jnp.zeros_like(dense)
    sub = lax.broadcasted_iota(jnp.int32, (SLOTS, 8, 128), 1)
    number = lax.broadcasted_iota(jnp.int32, (SLOTS, 8, 128), 0)
    copies[2].wait()
    which = ((0, 1, 2), (3, 4), (), (5,))
    for side, source in enumerate((own, other)):
        for column in range(COLS):
            tile = source[pl.ds(column * SLOTS, SLOTS)]
            total = tile
            for place, index in enumerate(which[column]):
                total = total + tile[:, 4 + place : 5 + place, :] * edge[index][None]
            first_slot = (core if side == 0 else 1 - core) * SLOTS
            live = (sub < 4) & (number < counts[column] - first_slot)
            total = jnp.where(live, total, 0.0)
            at = pl.ds((side * COLS + column) * SLOTS, SLOTS)
            staged[0, at] = total
            staged[1, at] = pltpu.roll(total, 4, 1)
    for copy in copies[:2]:
        copy.wait()
    for side, rows in enumerate((rows_own, rows_other)):
        for column in range(COLS):
            for slot in range(SLOTS):
                row = rows[column, slot]
                spot = base[row >> 5] + ((row >> 1) & 15)
                value = staged[row & 1, (side * COLS + column) * SLOTS + slot]
                dense[spot] = dense[spot] + value
    packed = []
    for column in range(16):
        after, before = [], []
        for tile in range(2):
            if column == 15:
                after.append(jnp.zeros((8, 128), jnp.float32))
            else:
                after.append(dense[base[column + 1] + tile])
            if column == 0:
                before.append(jnp.zeros((8, 128), jnp.float32))
            else:
                before.append(dense[base[column - 1] + 2 * NZ - 2 + tile])
        packed.append(pack_edges(after, before))
    for column in range(16):
        dense[base[column] + 2 * NZ] = packed[column]
    size = 4 * TILES
    for index, out in enumerate((out0, out1, out2, out3)):
        out[...] = dense[pl.ds(index * size, size)]


def scatter(counts, rows_own, rows_other, own, other, edge):
    size = 4 * TILES
    anywhere = pl.BlockSpec(memory_space=pl.ANY)
    vmem = pl.BlockSpec(memory_space=pltpu.VMEM)
    return pl.pallas_call(
        scatter_kernel,
        in_specs=[anywhere] * 3 + [vmem] * 3,
        out_specs=[vmem] * 4,
        out_shape=[jax.ShapeDtypeStruct((size, 8, 128), jnp.float32)] * 4,
        scratch_shapes=[
            pltpu.VMEM((4 * size, 8, 128), jnp.float32),
            pltpu.VMEM((2, 2 * HELD, 8, 128), jnp.float32),
            pltpu.SMEM((16,), jnp.int32),
            pltpu.SMEM((COLS,), jnp.int32),
            pltpu.SMEM((COLS, SLOTS), jnp.int32),
            pltpu.SMEM((COLS, SLOTS), jnp.int32),
            pltpu.SemaphoreType.DMA((3,)),
        ],
        compiler_params=pltpu.CompilerParams(vmem_limit_bytes=2 * SMALL),
        cost_estimate=pl.CostEstimate(flops=10**6, bytes_accessed=10**6, transcendentals=0),
        name="scatter",
    )(counts, rows_own, rows_other, own, other, edge)


def messages_kernel(part0, part1, part2, part3, out, total):
    total[0:TILES] = (part0[...] + part1[...]) + (part2[...] + part3[...])
    ends = unpack_edges(total[2 * NZ])
    for owner in range(NZ):
        here = 2 * owner
        out[owner, 0:2] = total[here : here + 2]
        after = ends if owner == NZ - 1 else (total[here + 2], total[here + 3])
        before = ends if owner == 0 else (total[here - 2], total[here - 1])
        out[owner, 2] = pack_edges(after, before)


def messages(parts):
    vmem = pl.BlockSpec(memory_space=pltpu.VMEM)
    return pl.pallas_call(
        messages_kernel,
        in_specs=[vmem] * 4,
        out_specs=vmem,
        out_shape=jax.ShapeDtypeStruct((NZ, 3, 8, 128), jnp.float32),
        scratch_shapes=[pltpu.VMEM((TILES, 8, 128), jnp.float32)],
        compiler_params=pltpu.CompilerParams(vmem_limit_bytes=SMALL),
        cost_estimate=pl.CostEstimate(flops=10**5, bytes_accessed=10**5, transcendentals=0),
        name="messages",
    )(*parts)


def inverse_kernel(density, mine, peer, out, turned, s3, s2, s1, s0, d3, d2, d1, even):
    x, y, z, core = coordinates()
    last = ((x * NY + y) * NZ + z) == OWNERS - 1
    inside = jnp.where(last, 0.0, 1.0)
    rows = []
    for half in (jnp.where(core == 0, mine[...], peer[...]), jnp.where(core == 0, peer[...], mine[...])):
        rows += [half[0:16], *unpack_edges(half[16:24])]
    both = jnp.concatenate(rows + [jnp.zeros((64, 128), jnp.float32)], axis=0)
    turned[...] = both.T

    def piece(half, block):
        return pltpu.roll(turned[...], (128 - (half * 32 + block * 4)) % 128, 1)

    def ghost(half, block, top):
        tile = turned[0:8, :] if top else turned[120:128, :]
        return pltpu.roll(tile, (128 - (half * 32 + 16 + block * 4)) % 128, 1)

    def fill(target, length, parts, left, right):
        for index, (half, block) in enumerate(parts):
            target[pl.ds(8 + index * 128, 128), :] = piece(half, block)
        if left is not None:
            target[0:8, :] = ghost(left[0], left[1], False)
        target[pl.ds(8 + length, 8), :] = ghost(right[0], right[1], True)

    fill(s3, 128, [(0, 0)], None, (0, 0))
    fill(d3, 128, [(1, 0)], (1, 0), (1, 0))
    fill(d2, 256, [(0, 1), (1, 1)], (1, 1), (0, 1))
    fill(d1, 512, [(0, 2), (1, 2), (0, 3), (1, 3)], (1, 3), (0, 2))

    def level(smooth, detail, length, target):
        for start in range(0, length, 128):
            value = smooth[pl.ds(8 + start, 128), :] - 0.25 * (
                detail[pl.ds(7 + start, 128), :] + detail[pl.ds(8 + start, 128), :]
            )
            even[pl.ds(start, 128), :] = value
            target[pl.ds(8 + 2 * start, 128, stride=2), :] = value
        tail = inside * (
            smooth[pl.ds(8 + length, 8), :]
            - 0.25 * (detail[pl.ds(7 + length, 8), :] + detail[pl.ds(8 + length, 8), :])
        )
        even[pl.ds(length, 8), :] = tail
        target[pl.ds(8 + 2 * length, 8), :] = tail
        for start in range(0, length, 128):
            value = detail[pl.ds(8 + start, 128), :] + 0.5 * (
                even[pl.ds(start, 128), :] + even[pl.ds(start + 1, 128), :]
            )
            target[pl.ds(9 + 2 * start, 128, stride=2), :] = value

    level(s3, d3, 128, s2)
    level(s2, d2, 256, s1)
    level(s1, d1, 512, s0)
    for group in range(8):
        at = pl.ds(group * 128, 128)
        out[:, at] = 0.5 * density[:, at] + s0[pl.ds(8 + group * 128, 128), :].T[0:4, :]


def inverse(density, mine, peer):
    vmem = pl.BlockSpec(memory_space=pltpu.VMEM)
    f32 = jnp.float32
    return pl.pallas_call(
        inverse_kernel,
        in_specs=[vmem] * 3,
        out_specs=vmem,
        out_shape=jax.ShapeDtypeStruct(density.shape, f32),
        scratch_shapes=[pltpu.VMEM((128, 128), f32)]
        + [pltpu.VMEM((n + 16, 128), f32) for n in (128, 256, 512, 1024, 128, 256, 512, 512)],
        compiler_params=pltpu.CompilerParams(vmem_limit_bytes=2 * SMALL),
        cost_estimate=pl.CostEstimate(flops=10**6, bytes_accessed=10**5, transcendentals=0),
        name="inverse",
    )(density, mine, peer)


def body(density, block_values, block_rows, block_counts):
    across = [(0, 1), (1, 0)]
    density, edge = stage(density)
    halo = lax.ppermute(edge, ALL, halo_pairs())
    rows_other = lax.ppermute(block_rows, "c", across)
    own, send = terms(density, block_values.reshape(HELD, BS, BS))
    received = lax.ppermute(send, "c", across)
    halo_other = lax.ppermute(halo, "c", across)
    edge_values = edges(density, halo, halo_other, jnp.asarray(edge_table()))
    parts = scatter(block_counts, block_rows, rows_other, own, received, edge_values)

    first = parts[0]
    for shift in (2, 1, 3):
        first = first + lax.ppermute(parts[shift], ALL, line_pairs(shift, False))
    first = first.reshape(4, TILES, 8, 128)
    second = [first[0]]
    for shift in (2, 1, 3):
        second.append(lax.ppermute(first[shift], ALL, line_pairs(shift, True)))
    last = lax.all_to_all(messages(second), "z", 0, 0, tiled=True).sum(axis=0)
    last = last.reshape(24, 128)
    return inverse(density, last, lax.ppermute(last, "c", across))


def solution(mesh):
    grid = Mesh(mesh.devices.reshape(NX, NY, NZ, NC), ALL)
    return jax.shard_map(
        body,
        mesh=grid,
        in_specs=(P(None, PATCH), P(PATCH, "c", None, None), P(PATCH, "c"), P(PATCH)),
        out_specs=P(None, PATCH),
        check_vma=False,
    )
```

```python
import jax
import jax.numpy as jnp
import numpy as np
from jax import lax
from jax.experimental import pallas as pl
from jax.experimental.pallas import tpu as pltpu
from jax.sharding import Mesh, PartitionSpec as P


LEVELS = 3
NX, NY, NZ, NC = 4, 4, 8, 2
PATCH = ("x", "y", "z")
ALL = ("x", "y", "z", "c")
OWNERS = NX * NY * NZ
TILES = 2 * NZ + 1
COLS, SLOTS, BS = 4, 16, 256
HELD = COLS * SLOTS
LEN = COLS * BS
REACH = 16
SMALL = 4 * 1024 * 1024


def device_id(x, y, z, c):
    return ((x * NY + y) * NZ + z) * NC + c


def halo_pairs():
    pairs = []
    for p in range(OWNERS):
        pairs.append((p * NC, ((p + 1) % OWNERS) * NC))
        pairs.append((p * NC + 1, ((p - 1) % OWNERS) * NC + 1))
    return pairs


def stage_kernel(density, staged, edge):
    core = lax.axis_index("c")
    value = density[...]
    staged[...] = value
    edge[...] = jnp.where(core == 0, value[:, LEN - 128 :], value[:, :128])


def stage(density):
    vmem = pl.BlockSpec(memory_space=pltpu.VMEM)
    return pl.pallas_call(
        stage_kernel,
        in_specs=[vmem],
        out_specs=[vmem, vmem],
        out_shape=[
            jax.ShapeDtypeStruct(density.shape, jnp.float32),
            jax.ShapeDtypeStruct((4, 128), jnp.float32),
        ],
        compiler_params=pltpu.CompilerParams(vmem_limit_bytes=SMALL),
        name="stage",
    )(density)


def pack_edges(after, before):
    lane = lax.broadcasted_iota(jnp.int32, (8, 128), 1)
    tiles = [jnp.where(lane < 64, high, low) for high, low in zip(after, before)]
    return jnp.where((lane >= 16) & (lane < 48), pltpu.roll(tiles[1], 32, 1), tiles[0])


def unpack_edges(tile):
    return tile, pltpu.roll(tile, 96, 1)


def line_pairs(shift, swap):
    pairs = []
    for x in range(NX):
        for y in range(NY):
            for z in range(NZ):
                for c in range(NC):
                    if (c == 0) != swap:
                        target = device_id((x + shift) % NX, y, z, c)
                    else:
                        target = device_id(x, (y + shift) % NY, z, c)
                    pairs.append((device_id(x, y, z, c), target))
    return pairs


def edge_table():
    table = np.zeros((128, 128), np.float32)
    for at_end in (False, True):
        for unit in range(64):
            line = np.zeros(LEN + 2 * REACH)
            where = unit if unit < 32 else LEN + unit - 32
            line[where] = 1.0
            if at_end:
                line[:REACH] = 0.0
                line[REACH + LEN :] = 0.0
            smooth, details = line, []
            for level in range(LEVELS):
                margin, length = REACH >> (level + 1), LEN >> (level + 1)
                keep = np.ones(length + 2 * margin)
                if at_end:
                    keep[:margin] = 0.0
                    keep[margin + length :] = 0.0
                even, odd = smooth[0::2], smooth[1::2]
                detail = (odd - 0.5 * (even + np.append(even[1:], 0.0))) * keep
                smooth = (even + 0.25 * (np.append(0.0, detail[:-1]) + detail)) * keep
                details.append(detail[margin : margin + length])
            s3 = smooth[margin : margin + length]
            d1, d2, d3 = details
            values = [s3[0], d3[0], d3[127], d2[0], d2[255], d1[511]]
            table[unit, 8 * at_end : 8 * at_end + 6] = values
    return table


def coordinates():
    return [lax.axis_index(axis) for axis in ALL]


CHUNKS = {0: 4, 4: 12, 16: 16, 32: 16, 48: 16}


def terms_kernel(density, values, own, send, wide, xt, d1, s1, d2, s2, d3, vec, acc, held, sems):
    core = lax.axis_index("c")
    copies = {
        at: pltpu.make_async_copy(values.at[pl.ds(at, size)], held.at[pl.ds(at, size)], sems.at[i])
        for i, (at, size) in enumerate(CHUNKS.items())
    }
    for copy in copies.values():
        copy.start()
    wide[0:4, :] = density[...]
    wide[4:8, :] = density[...]
    for group in range(8):
        tile = wide[:, pl.ds(group * 128, 128)]
        xt[pl.ds(8 + group * 128, 128), :] = jnp.concatenate([tile] * 16, axis=0).T
    pad = jnp.zeros((8, 128), jnp.float32)

    def lift(source, length, detail, smooth, fix):
        source[pl.ds(8 + 2 * length, 8), :] = pad
        detail[0:8, :] = pad
        step = min(length, 128)
        for start in range(0, length, step):
            even = source[pl.ds(8 + 2 * start, step, stride=2), :]
            odd = source[pl.ds(9 + 2 * start, step, stride=2), :]
            after = source[pl.ds(10 + 2 * start, step, stride=2), :]
            detail[pl.ds(8 + start, step), :] = odd - 0.5 * (even + after)
        if fix:
            row = lax.broadcasted_iota(jnp.int32, (8, 128), 0)
            detail[8:16, :] = jnp.where(row == 0, 0.0, detail[8:16, :])
            detail[pl.ds(length, 8), :] = jnp.where(row == 7, 0.0, detail[pl.ds(length, 8), :])
        for start in range(0, length, step):
            even = source[pl.ds(8 + 2 * start, step, stride=2), :]
            low = detail[pl.ds(7 + start, step), :]
            high = detail[pl.ds(8 + start, step), :]
            smooth(start, step, even + 0.25 * (low + high))

    lane = lax.broadcasted_iota(jnp.int32, (8, 128), 1) & 7
    row = lax.broadcasted_iota(jnp.int32, (8, 128), 0)

    def put(at, value):
        count = value.shape[0]
        lanes = lax.broadcasted_iota(jnp.int32, (count, 128), 1) & 7
        vec[pl.ds(at, count), :] = jnp.where(lanes < 4, value, 0.0)

    def keep1(start, step, value):
        s1[pl.ds(8 + start, step), :] = value

    def keep2(start, step, value):
        s2[pl.ds(8 + start, step), :] = value

    lift(xt, 512, d1, keep1, False)
    lift(s1, 256, d2, keep2, False)
    lift(s2, 128, d3, lambda start, step, value: put(start, value), True)
    put(128, d3[8:136, :])
    put(256, d2[8:264, :])
    for start in range(0, 512, 128):
        put(512 + start, d1[pl.ds(8 + start, 128), :])

    def patch(at, which, lanes_weights, clear):
        tile = vec[pl.ds(at, 8), :]
        if clear:
            tile = jnp.where((row == which) & (lane < 4), 0.0, tile)
        for index, at_row, weight in lanes_weights:
            tile = jnp.where((row == at_row) & (lane == index), weight, tile)
        vec[pl.ds(at, 8), :] = tile

    patch(0, 0, [(4, 0, 1.0), (5, 1, 0.25)], True)
    patch(120, 7, [(6, 7, 0.25)], False)
    patch(128, 0, [(5, 0, 1.0)], True)
    patch(248, 7, [(6, 7, 1.0)], True)
    patch(256, 0, [(4, 0, 1.0)], True)
    patch(504, 7, [(5, 7, 1.0)], True)
    patch(1016, 7, [(4, 7, 1.0)], True)

    whose = lax.broadcasted_iota(jnp.int32, (1, 128), 1) >> 3
    for column in range(COLS):
        vector = vec[pl.ds(column * BS, BS), :].astype(jnp.bfloat16)
        for slot in range(SLOTS):
            index = column * SLOTS + slot
            if index in copies:
                copies[index].wait()
            mask = (whose == slot).astype(jnp.float32).astype(jnp.bfloat16)
            part = jnp.dot(held[index], vector * mask, preferred_element_type=jnp.float32)
            if slot == 0:
                acc[...] = part
            else:
                acc[...] += part
        turned = acc[...].T
        low = turned[:, :128].reshape(SLOTS, 8, 128)
        high = turned[:, 128:].reshape(SLOTS, 8, 128)
        at = pl.ds(column * SLOTS, SLOTS)
        own[at] = jnp.where(core == 0, low, high)
        send[at] = jnp.where(core == 0, high, low)


def terms(density, values):
    vmem = pl.BlockSpec(memory_space=pltpu.VMEM)
    block = jax.ShapeDtypeStruct((HELD, 8, 128), jnp.float32)
    f32 = jnp.float32
    return pl.pallas_call(
        terms_kernel,
        in_specs=[vmem, pl.BlockSpec(memory_space=pltpu.HBM)],
        out_specs=[vmem, vmem],
        out_shape=[block, block],
        scratch_shapes=[
            pltpu.VMEM((8, LEN), f32),
            pltpu.VMEM((LEN + 16, 128), f32),
            pltpu.VMEM((512 + 16, 128), f32),
            pltpu.VMEM((512 + 16, 128), f32),
            pltpu.VMEM((256 + 16, 128), f32),
            pltpu.VMEM((256 + 16, 128), f32),
            pltpu.VMEM((128 + 16, 128), f32),
            pltpu.VMEM((LEN, 128), f32),
            pltpu.VMEM((BS, 128), f32),
            pltpu.VMEM((HELD, BS, BS), jnp.bfloat16),
            pltpu.SemaphoreType.DMA((len(CHUNKS),)),
        ],
        compiler_params=pltpu.CompilerParams(vmem_limit_bytes=50 * 1024 * 1024),
        cost_estimate=pl.CostEstimate(
            flops=2 * HELD * BS * BS * 128, bytes_accessed=2 * HELD * BS * BS, transcendentals=0
        ),
        name="terms",
    )(density, values)


def edges_kernel(density, mine, other, table, out):
    x, y, z, core = coordinates()
    left = jnp.where(core == 0, mine[...], other[...])
    right = jnp.where(core == 0, other[...], mine[...])
    lane = lax.broadcasted_iota(jnp.int32, (4, 128), 1)
    first = density[:, 0:128]
    last = density[:, LEN - 128 :]
    inputs = jnp.where(
        lane < 32,
        jnp.where(lane < 16, pltpu.roll(left, 16, 1), pltpu.roll(first, 16, 1)),
        jnp.where(lane < 48, pltpu.roll(last, 48, 1), pltpu.roll(right, 48, 1)),
    )
    inputs = jnp.where(lane < 64, inputs, 0.0)
    values = jnp.dot(
        inputs, table[...], precision=lax.Precision.HIGHEST, preferred_element_type=jnp.float32
    )
    patch = (x * NY + y) * NZ + z
    low = (lane == 0) | (lane == 1) | (lane == 3)
    at_end = jnp.where(low, (patch == 0).astype(jnp.int32), (patch == OWNERS - 1).astype(jnp.int32))
    values = jnp.where(at_end == 1, pltpu.roll(values, 120, 1), values)
    values = values.astype(jnp.bfloat16).astype(jnp.float32)
    for index in range(6):
        spread = jnp.broadcast_to(values[:, index : index + 1], (4, 128))
        out[index, 0:4, :] = spread
        out[index, 4:8, :] = jnp.zeros((4, 128), jnp.float32)


def edges(density, mine, other, table):
    vmem = pl.BlockSpec(memory_space=pltpu.VMEM)
    return pl.pallas_call(
        edges_kernel,
        in_specs=[vmem] * 4,
        out_specs=vmem,
        out_shape=jax.ShapeDtypeStruct((6, 8, 128), jnp.float32),
        compiler_params=pltpu.CompilerParams(vmem_limit_bytes=SMALL),
        cost_estimate=pl.CostEstimate(flops=10**6, bytes_accessed=10**5, transcendentals=0),
        name="edges",
    )(density, mine, other, table)


def scatter_kernel(
    counts_ref,
    rows_ref,
    rows_other_ref,
    own,
    other,
    edge,
    *refs,
):
    outs, (dense, staged, base, counts, rows_own, rows_other, sems) = refs[:8], refs[8:]
    x, y, _, core = coordinates()
    copies = [
        pltpu.make_async_copy(rows_ref, rows_own, sems.at[0]),
        pltpu.make_async_copy(rows_other_ref, rows_other, sems.at[1]),
        pltpu.make_async_copy(counts_ref, counts, sems.at[2]),
    ]
    for copy in copies:
        copy.start()

    def relative(column_x, column_y):
        dx, dy = (column_x - x) & 3, (column_y - y) & 3
        return jnp.where(core == 0, dx * 4 + dy, dy * 4 + dx)

    for column in range(16):
        base[column] = relative(column >> 2, column & 3) * TILES
    dense[...] = jnp.zeros_like(dense)
    sub = lax.broadcasted_iota(jnp.int32, (SLOTS, 8, 128), 1)
    which = ((0, 1, 2), (3, 4), (), (5,))
    for side, source in enumerate((own, other)):
        for column in range(COLS):
            tile = source[pl.ds(column * SLOTS, SLOTS)]
            total = tile
            for place, index in enumerate(which[column]):
                total = total + tile[:, 4 + place : 5 + place, :] * edge[index][None]
            total = jnp.where(sub < 4, total, 0.0)
            at = pl.ds((side * COLS + column) * SLOTS, SLOTS)
            staged[0, at] = total
            staged[1, at] = pltpu.roll(total, 4, 1)
    for copy in copies:
        copy.wait()
    spare = 16 * TILES
    for side, rows in enumerate((rows_own, rows_other)):
        for column in range(COLS):
            live = counts[column] - (core if side == 0 else 1 - core) * SLOTS
            for slot in range(SLOTS):
                row = rows[column, slot]
                spot = jnp.where(slot < live, base[row >> 5] + ((row >> 1) & 15), spare)
                value = staged[row & 1, (side * COLS + column) * SLOTS + slot]
                dense[spot] = dense[spot] + value
    packed = []
    for column in range(16):
        after, before = [], []
        for tile in range(2):
            if column == 15:
                after.append(jnp.zeros((8, 128), jnp.float32))
            else:
                after.append(dense[base[column + 1] + tile])
            if column == 0:
                before.append(jnp.zeros((8, 128), jnp.float32))
            else:
                before.append(dense[base[column - 1] + 2 * NZ - 2 + tile])
        packed.append(pack_edges(after, before))
    for column in range(16):
        dense[base[column] + 2 * NZ] = packed[column]
    size = 4 * TILES
    for index in range(4):
        outs[2 * index][...] = dense[pl.ds(index * size + TILES, 3 * TILES)]
        outs[2 * index + 1][...] = dense[pl.ds(index * size, TILES)]


def scatter(counts, rows_own, rows_other, own, other, edge):
    size = 4 * TILES
    anywhere = pl.BlockSpec(memory_space=pl.ANY)
    vmem = pl.BlockSpec(memory_space=pltpu.VMEM)
    return pl.pallas_call(
        scatter_kernel,
        in_specs=[anywhere] * 3 + [vmem] * 3,
        out_specs=[vmem] * 8,
        out_shape=[jax.ShapeDtypeStruct((count * TILES, 8, 128), jnp.float32) for count in (3, 1)] * 4,
        scratch_shapes=[
            pltpu.VMEM((4 * size + 1, 8, 128), jnp.float32),
            pltpu.VMEM((2, 2 * HELD, 8, 128), jnp.float32),
            pltpu.SMEM((16,), jnp.int32),
            pltpu.SMEM((COLS,), jnp.int32),
            pltpu.SMEM((COLS, SLOTS), jnp.int32),
            pltpu.SMEM((COLS, SLOTS), jnp.int32),
            pltpu.SemaphoreType.DMA((3,)),
        ],
        compiler_params=pltpu.CompilerParams(vmem_limit_bytes=2 * SMALL),
        cost_estimate=pl.CostEstimate(flops=10**6, bytes_accessed=10**6, transcendentals=0),
        name="scatter",
    )(counts, rows_own, rows_other, own, other, edge)


def messages_kernel(*refs):
    parts, out, total = refs[:-2], refs[-2], refs[-1]
    value = parts[0][...]
    for part in parts[1:]:
        value = value + part[...]
    total[...] = value
    ends = unpack_edges(total[2 * NZ])
    for owner in range(NZ):
        here = 2 * owner
        out[owner, 0:2] = total[here : here + 2]
        after = ends if owner == NZ - 1 else (total[here + 2], total[here + 3])
        before = ends if owner == 0 else (total[here - 2], total[here - 1])
        out[owner, 2] = pack_edges(after, before)


def messages(parts):
    vmem = pl.BlockSpec(memory_space=pltpu.VMEM)
    return pl.pallas_call(
        messages_kernel,
        in_specs=[vmem] * len(parts),
        out_specs=vmem,
        out_shape=jax.ShapeDtypeStruct((NZ, 3, 8, 128), jnp.float32),
        scratch_shapes=[pltpu.VMEM((TILES, 8, 128), jnp.float32)],
        compiler_params=pltpu.CompilerParams(vmem_limit_bytes=SMALL),
        cost_estimate=pl.CostEstimate(flops=10**5, bytes_accessed=10**5, transcendentals=0),
        name="messages",
    )(*parts)


def inverse_kernel(density, mine, peer, out, turned, s3, s2, s1, s0, d3, d2, d1, even):
    x, y, z, core = coordinates()
    last = ((x * NY + y) * NZ + z) == OWNERS - 1
    inside = jnp.where(last, 0.0, 1.0)
    rows = []
    for half in (jnp.where(core == 0, mine[...], peer[...]), jnp.where(core == 0, peer[...], mine[...])):
        rows += [half[0:16], *unpack_edges(half[16:24])]
    both = jnp.concatenate(rows + [jnp.zeros((64, 128), jnp.float32)], axis=0)
    turned[...] = both.T

    def piece(half, block):
        return pltpu.roll(turned[...], (128 - (half * 32 + block * 4)) % 128, 1)

    def ghost(half, block, top):
        tile = turned[0:8, :] if top else turned[120:128, :]
        return pltpu.roll(tile, (128 - (half * 32 + 16 + block * 4)) % 128, 1)

    def fill(target, length, parts, left, right):
        for index, (half, block) in enumerate(parts):
            target[pl.ds(8 + index * 128, 128), :] = piece(half, block)
        if left is not None:
            target[0:8, :] = ghost(left[0], left[1], False)
        target[pl.ds(8 + length, 8), :] = ghost(right[0], right[1], True)

    fill(s3, 128, [(0, 0)], None, (0, 0))
    fill(d3, 128, [(1, 0)], (1, 0), (1, 0))
    fill(d2, 256, [(0, 1), (1, 1)], (1, 1), (0, 1))
    fill(d1, 512, [(0, 2), (1, 2), (0, 3), (1, 3)], (1, 3), (0, 2))

    def level(smooth, detail, length, target):
        for start in range(0, length, 128):
            value = smooth[pl.ds(8 + start, 128), :] - 0.25 * (
                detail[pl.ds(7 + start, 128), :] + detail[pl.ds(8 + start, 128), :]
            )
            even[pl.ds(start, 128), :] = value
            target[pl.ds(8 + 2 * start, 128, stride=2), :] = value
        tail = inside * (
            smooth[pl.ds(8 + length, 8), :]
            - 0.25 * (detail[pl.ds(7 + length, 8), :] + detail[pl.ds(8 + length, 8), :])
        )
        even[pl.ds(length, 8), :] = tail
        target[pl.ds(8 + 2 * length, 8), :] = tail
        for start in range(0, length, 128):
            value = detail[pl.ds(8 + start, 128), :] + 0.5 * (
                even[pl.ds(start, 128), :] + even[pl.ds(start + 1, 128), :]
            )
            target[pl.ds(9 + 2 * start, 128, stride=2), :] = value

    level(s3, d3, 128, s2)
    level(s2, d2, 256, s1)
    level(s1, d1, 512, s0)
    for group in range(8):
        at = pl.ds(group * 128, 128)
        out[:, at] = 0.5 * density[:, at] + s0[pl.ds(8 + group * 128, 128), :].T[0:4, :]


def inverse(density, mine, peer):
    vmem = pl.BlockSpec(memory_space=pltpu.VMEM)
    f32 = jnp.float32
    return pl.pallas_call(
        inverse_kernel,
        in_specs=[vmem] * 3,
        out_specs=vmem,
        out_shape=jax.ShapeDtypeStruct(density.shape, f32),
        scratch_shapes=[pltpu.VMEM((128, 128), f32)]
        + [pltpu.VMEM((n + 16, 128), f32) for n in (128, 256, 512, 1024, 128, 256, 512, 512)],
        compiler_params=pltpu.CompilerParams(vmem_limit_bytes=2 * SMALL),
        cost_estimate=pl.CostEstimate(flops=10**6, bytes_accessed=10**5, transcendentals=0),
        name="inverse",
    )(density, mine, peer)


def body(density, block_values, block_rows, block_counts):
    across = [(0, 1), (1, 0)]
    density, edge = stage(density)
    halo = lax.ppermute(edge, ALL, halo_pairs())
    rows_other = lax.ppermute(block_rows, "c", across)
    own, send = terms(density, block_values.reshape(HELD, BS, BS))
    received = lax.ppermute(send, "c", across)
    halo_other = lax.ppermute(halo, "c", across)
    edge_values = edges(density, halo, halo_other, jnp.asarray(edge_table()))
    parts = scatter(block_counts, block_rows, rows_other, own, received, edge_values)

    onward, mine = parts[0::2], parts[1::2]
    arrived, kept = [onward[0]], [mine[0]]
    for shift in (2, 1, 3):
        arrived.append(lax.ppermute(onward[shift], ALL, line_pairs(shift, False)))
    for shift in (2, 1, 3):
        kept.append(lax.ppermute(mine[shift], ALL, line_pairs(shift, False)))
    first = sum(arrived[1:], arrived[0]).reshape(3, TILES, 8, 128)
    for shift in (2, 1, 3):
        kept.append(lax.ppermute(first[shift - 1], ALL, line_pairs(shift, True)))
    second = kept
    last = lax.all_to_all(messages(second), "z", 0, 0, tiled=True).sum(axis=0)
    last = last.reshape(24, 128)
    return inverse(density, last, lax.ppermute(last, "c", across))


def solution(mesh):
    grid = Mesh(mesh.devices.reshape(NX, NY, NZ, NC), ALL)
    return jax.shard_map(
        body,
        mesh=grid,
        in_specs=(P(None, PATCH), P(PATCH, "c", None, None), P(PATCH, "c"), P(PATCH)),
        out_specs=P(None, PATCH),
        check_vma=False,
    )
```
